32 devices in a mesh: dp: 8 (over z, y), query: 4 (over x, core).
Axes of the slice: x: 2, y: 2, z: 4, core: 2. Of those that a mesh axis runs over, the one named last changes fastest.
Arguments:
- sensors: bfloat16 [3072, 4096], P('dp'), may hold values from -8 to 8
- query_index: int32 [2, 8192], P(None, 'query'), may hold values from 0 to 127
- targets: bfloat16 [3072, 8192], P('dp', 'query'), may hold values from -6 to 6
- w_one: bfloat16 [4096, 1024], P(None, 'query'), may hold values from -0.09375 to 0.09375
- b_one: float32 [1024], P('query'), may hold values from -3 to 3
- w_two: bfloat16 [1024, 512], P('query'), may hold values from -0.1875 to 0.1875
- b_two: float32 [512], replicated, may hold values from -3 to 3
- v_one: float32 [2, 512], replicated, may hold values from -4 to 4
- c_one: float32 [512], replicated, may hold values from -3 to 3
- v_two: bfloat16 [512, 512], replicated, may hold values from -0.25 to 0.25
- c_two: float32 [512], replicated, may hold values from -3 to 3
- v_three: bfloat16 [512, 512], replicated, may hold values from -0.25 to 0.25
- c_three: float32 [512], replicated, may hold values from -3 to 3
Outputs:
- loss: float32 [], replicated
- grad_w_one: float32 [4096, 1024], P('dp', 'query')
- grad_b_one: float32 [1024], P('query')
- grad_w_two: float32 [1024, 512], P('query', 'dp')
- grad_b_two: float32 [512], replicated
- grad_v_one: float32 [2, 512], replicated
- grad_c_one: float32 [512], replicated
- grad_v_two: float32 [512, 512], replicated
- grad_c_two: float32 [512], replicated
- grad_v_three: float32 [512, 512], replicated
- grad_c_three: float32 [512], replicated
The draws below stay inside these ranges and needn't reach their ends.
All inputs are finite; a program needn't handle non-finite values.
Results may differ from the reference program's by a relative error of at most 0.00075.
Values may be sent and summed in bfloat16 or wider, within the bound.
A program may use at most 128 MiB of HBM per device.

```python
import math
import jax
import jax.numpy as jnp
from jax import lax

SENSORS = 4096
HIDDEN_SIZE = 1024
BASIS = 512
TRUNK = 512
GRID = 128
FUNC_DEV = 384
FUNCS = 3072
QUERIES = 8192
N_DP = 8


latent_count = 8


def joint_fields(key):
    key_latent = jax.random.fold_in(key, 7101)
    key_sdirs = jax.random.fold_in(key, 7102)
    key_qdirs = jax.random.fold_in(key, 7103)
    key_snoise = jax.random.fold_in(key, 7104)
    key_tnoise = jax.random.fold_in(key, 7105)
    key_pairs = jax.random.fold_in(key, 7107)
    latent = jax.random.normal(key_latent, (FUNCS, latent_count), jnp.float32)
    sensor_dirs = jax.random.normal(key_sdirs, (latent_count, SENSORS), jnp.float32)
    query_dirs = jax.random.normal(key_qdirs, (latent_count, QUERIES), jnp.float32)
    sensor_noise = jax.random.normal(key_snoise, (FUNCS, SENSORS), jnp.float32)
    target_noise = jax.random.normal(key_tnoise, (FUNCS, QUERIES), jnp.float32)
    noise_share = 0.5
    pairing = jax.random.permutation(key_pairs, N_DP)
    func_block = jnp.arange(FUNCS, dtype=jnp.int32) // FUNC_DEV
    sensor_block = jnp.arange(SENSORS, dtype=jnp.int32) // (SENSORS // N_DP)
    spiked = pairing[func_block][:, None] == sensor_block[None, :]
    boost = jnp.where(spiked, 3.0, 1.0).astype(jnp.float32)
    mixed = jnp.dot(latent, sensor_dirs) * (0.9 / math.sqrt(latent_count))
    sensors = jnp.clip(0.5 * boost * sensor_noise + mixed, -8.0, 8.0)
    solution = jnp.dot(latent, query_dirs) * (1.0 / math.sqrt(latent_count))
    targets = jnp.clip(solution + noise_share * target_noise, -6.0, 6.0)
    return (sensors, targets)


def draw_sensors(key, part):
    return joint_fields(key)[0].astype(jnp.bfloat16)


def draw_targets(key, part):
    return joint_fields(key)[1].astype(jnp.bfloat16)


def with_ends(drawn, rng, smallest, largest):
    spot = [jax.random.randint(jax.random.fold_in(rng, axis), (), 0, length) for axis, length in enumerate(drawn.shape)]
    widest = drawn.shape.index(max(drawn.shape))
    neighbour = spot[:widest] + [(spot[widest] + 1) % drawn.shape[widest]] + spot[widest + 1:]
    return drawn.at[tuple(spot)].set(smallest).at[tuple(neighbour)].set(largest)


def shard_levels(own_key, extent, split, smallest, high):
    def one(dim, parts):
        steps = jax.random.uniform(jax.random.fold_in(jax.random.fold_in(own_key, 6), dim), (parts,), jnp.float32, smallest / len(split), high / len(split))
        return jnp.repeat(jnp.exp(steps), extent[dim] // parts).reshape((-1,) + (1,) * (len(extent) - dim - 1))

    gain = one(*split[0])
    for cut in split[1:]:
        gain = gain * one(*cut)
    return gain


def normal_values(stream_key, extent, spread, reach, cuts=(), held_as=jnp.bfloat16):
    entries = spread * jax.random.normal(stream_key, extent, jnp.float32)
    if cuts:
        entries = entries * shard_levels(stream_key, extent, cuts, -0.22, 0.18)
    return jnp.clip(entries, -reach, reach).astype(held_as)


def setup_inputs(seed: int = 0) -> dict:
    streams_of = jax.random.split(jax.random.key(seed), 14)
    sensors = draw_sensors(jax.random.fold_in(streams_of[13], 71), 0)
    query_index = with_ends(jax.random.randint(streams_of[1], (2, QUERIES), 0, GRID), jax.random.fold_in(streams_of[1], 1), 0, GRID - 1).astype(jnp.int32)
    targets = draw_targets(jax.random.fold_in(streams_of[13], 71), 0)
    w_one = normal_values(streams_of[3], (SENSORS, HIDDEN_SIZE), SENSORS ** -0.5, 0.09375, ((1, 4),))
    b_one = normal_values(streams_of[4], (HIDDEN_SIZE,), 0.5, 3.0, ((0, 4),), jnp.float32)
    w_two = normal_values(streams_of[5], (HIDDEN_SIZE, BASIS), HIDDEN_SIZE ** -0.5, 0.1875, ((0, 4),))
    b_two = normal_values(streams_of[6], (BASIS,), 0.5, 3.0, (), jnp.float32)
    v_one = normal_values(streams_of[7], (2, TRUNK), 2 ** -0.5, 4.0, (), jnp.float32)
    c_one = normal_values(streams_of[8], (TRUNK,), 0.5, 3.0, (), jnp.float32)
    v_two = normal_values(streams_of[9], (TRUNK, TRUNK), TRUNK ** -0.5, 0.25)
    c_two = normal_values(streams_of[10], (TRUNK,), 0.5, 3.0, (), jnp.float32)
    v_three = normal_values(streams_of[11], (TRUNK, BASIS), TRUNK ** -0.5, 0.25)
    c_three = normal_values(streams_of[12], (BASIS,), 0.5, 3.0, (), jnp.float32)
    return {"sensors": sensors, "query_index": query_index, "targets": targets, "w_one": w_one, "b_one": b_one, "w_two": w_two, "b_two": b_two, "v_one": v_one, "c_one": c_one, "v_two": v_two, "c_two": c_two, "v_three": v_three, "c_three": c_three}


def contract_rows(left, right, precision=None):
    return lax.dot_general(left, right, (((0,), (0,)), ((), ())), precision=precision, preferred_element_type=jnp.float32)

def contract_cols(left, right, precision=None):
    return lax.dot_general(left, right, (((1,), (1,)), ((), ())), precision=precision, preferred_element_type=jnp.float32)

def trunk_forward(coords, v_one, c_one, v_two, c_two, v_three, c_three):
    first_act = jnp.tanh(coords[0][:, None] * v_one[0][None, :] + coords[1][:, None] * v_one[1][None, :] + c_one)
    first_b = first_act.astype(jnp.bfloat16)
    second_act = jnp.tanh(jnp.dot(first_b, v_two, preferred_element_type=jnp.float32) + c_two)
    second_b = second_act.astype(jnp.bfloat16)
    basis_full = jnp.dot(second_b, v_three, preferred_element_type=jnp.float32) + c_three
    return (first_act, first_b, second_act, second_b, basis_full.astype(jnp.bfloat16))

def trunk_backward(coords, first_act, first_b, second_act, second_b, grad_basis, v_two, v_three):
    grad_basis_b = grad_basis.astype(jnp.bfloat16)
    grad_v_three = contract_rows(second_b, grad_basis_b)
    grad_c_three = lax.optimization_barrier(jnp.sum(grad_basis, axis=0))
    grad_second = contract_cols(grad_basis_b, v_three) * (1.0 - second_act * second_act)
    grad_second_b = grad_second.astype(jnp.bfloat16)
    grad_v_two = contract_rows(first_b, grad_second_b)
    grad_c_two = lax.optimization_barrier(jnp.sum(grad_second, axis=0))
    grad_first = contract_cols(grad_second_b, v_two) * (1.0 - first_act * first_act)
    grad_v_one = jnp.dot(coords, grad_first, precision=lax.Precision.HIGHEST, preferred_element_type=jnp.float32)
    grad_c_one = lax.optimization_barrier(jnp.sum(grad_first, axis=0))
    return (grad_v_one, grad_c_one, grad_v_two, grad_c_two, grad_v_three, grad_c_three)

def reference(sensors, query_index, targets, w_one, b_one, w_two, b_two, v_one, c_one, v_two, c_two, v_three, c_three):
    coords = query_index.astype(jnp.float32) / (GRID - 1)
    first_act, first_b, second_act, second_b, basis_b = trunk_forward(coords, v_one, c_one, v_two, c_two, v_three, c_three)
    inv_scale = 1.0 / math.sqrt(BASIS)
    grad_scale = 64.0 / math.sqrt(FUNCS * QUERIES)
    sens_blocks = sensors.reshape(N_DP, FUNC_DEV, SENSORS)
    target_blocks = targets.reshape(N_DP, FUNC_DEV, QUERIES)

    def accumulate(running, block):
        loss_sum, grad_basis, grad_w_one, grad_b_one, grad_w_two, grad_b_two = running
        sens_block, target_block = block
        hidden = jnp.tanh(jnp.dot(sens_block, w_one, preferred_element_type=jnp.float32) + b_one)
        hidden_b = hidden.astype(jnp.bfloat16)
        coeffs = jnp.dot(hidden_b, w_two, preferred_element_type=jnp.float32) + b_two
        coeffs_b = coeffs.astype(jnp.bfloat16)
        prediction = contract_cols(coeffs_b, basis_b) * inv_scale
        misfit = prediction - target_block.astype(jnp.float32)
        loss_sum = loss_sum + jnp.sum(misfit * misfit)
        misfit_b = (misfit * grad_scale).astype(jnp.bfloat16)
        grad_coeffs = jnp.dot(misfit_b, basis_b, preferred_element_type=jnp.float32) * inv_scale
        grad_coeffs_b = grad_coeffs.astype(jnp.bfloat16)
        grad_basis = grad_basis + contract_rows(misfit_b, coeffs_b) * inv_scale
        grad_b_two = grad_b_two + lax.optimization_barrier(jnp.sum(grad_coeffs, axis=0))
        grad_w_two = grad_w_two + contract_rows(hidden_b, grad_coeffs_b)
        grad_pre = contract_cols(grad_coeffs_b, w_two) * (1.0 - hidden * hidden)
        grad_b_one = grad_b_one + lax.optimization_barrier(jnp.sum(grad_pre, axis=0))
        grad_w_one = grad_w_one + contract_rows(sens_block, grad_pre.astype(jnp.bfloat16))
        return ((loss_sum, grad_basis, grad_w_one, grad_b_one, grad_w_two, grad_b_two), None)
    initial = (jnp.zeros((), jnp.float32), jnp.zeros((QUERIES, BASIS), jnp.float32), jnp.zeros((SENSORS, HIDDEN_SIZE), jnp.float32), jnp.zeros((HIDDEN_SIZE,), jnp.float32), jnp.zeros((HIDDEN_SIZE, BASIS), jnp.float32), jnp.zeros((BASIS,), jnp.float32))
    final, _ = lax.scan(accumulate, initial, (sens_blocks, target_blocks))
    loss_sum, grad_basis, grad_w_one, grad_b_one, grad_w_two, grad_b_two = final
    grad_v_one, grad_c_one, grad_v_two, grad_c_two, grad_v_three, grad_c_three = trunk_backward(coords, first_act, first_b, second_act, second_b, grad_basis, v_two, v_three)
    return (loss_sum / (FUNCS * QUERIES), grad_w_one, grad_b_one, grad_w_two, grad_b_two, grad_v_one, grad_c_one, grad_v_two, grad_c_two, grad_v_three, grad_c_three)
```

```python
import math

import jax
import jax.numpy as jnp
from jax import lax
from jax.sharding import PartitionSpec as P

GRID = 128


def contract_rows(left, right, precision=None):
    return lax.dot_general(
        left,
        right,
        (((0,), (0,)), ((), ())),
        precision=precision,
        preferred_element_type=jnp.float32,
    )


def contract_cols(left, right, precision=None):
    return lax.dot_general(
        left,
        right,
        (((1,), (1,)), ((), ())),
        precision=precision,
        preferred_element_type=jnp.float32,
    )


def trunk_forward(coords, v_one, c_one, v_two, c_two, v_three, c_three):
    first_act = jnp.tanh(
        coords[0][:, None] * v_one[0][None, :] + coords[1][:, None] * v_one[1][None, :] + c_one
    )
    first_b = first_act.astype(jnp.bfloat16)
    second_act = jnp.tanh(jnp.dot(first_b, v_two, preferred_element_type=jnp.float32) + c_two)
    second_b = second_act.astype(jnp.bfloat16)
    basis_full = jnp.dot(second_b, v_three, preferred_element_type=jnp.float32) + c_three
    return (first_act, first_b, second_act, second_b, basis_full.astype(jnp.bfloat16))


def swap(value, axis, mask):
    count = lax.axis_size(axis)
    return lax.ppermute(value, axis, [(i, i ^ mask) for i in range(count)])


def bits_of(count):
    return [1 << b for b in range(count.bit_length() - 1)]


def gather_xor(value, axis, masks):
    blocks, offsets = value, [0]
    for mask in masks:
        blocks = jnp.concatenate([blocks, swap(blocks, axis, mask)], axis=0)
        offsets = offsets + [o ^ mask for o in offsets]
    return blocks, offsets


def split_pair(value):
    high = lax.reduce_precision(value, 8, 7)
    return high.astype(jnp.bfloat16), (value - high).astype(jnp.bfloat16)


def trunk_backward(coords, first_act, first_b, second_act, second_b, grad_basis, v_two, v_three):
    basis_hi, basis_lo = split_pair(grad_basis)
    grad_v_three = contract_rows(second_b, basis_hi) + contract_rows(second_b, basis_lo)
    grad_c_three = jnp.sum(grad_basis, axis=0)
    grad_second = (contract_cols(basis_hi, v_three) + contract_cols(basis_lo, v_three)) * (
        1.0 - second_act * second_act
    )
    second_hi, second_lo = split_pair(grad_second)
    grad_v_two = contract_rows(first_b, second_hi) + contract_rows(first_b, second_lo)
    grad_c_two = jnp.sum(grad_second, axis=0)
    grad_first = (contract_cols(second_hi, v_two) + contract_cols(second_lo, v_two)) * (
        1.0 - first_act * first_act
    )
    grad_v_one = jnp.stack(
        [jnp.sum(coords[0][:, None] * grad_first, axis=0), jnp.sum(coords[1][:, None] * grad_first, axis=0)]
    )
    grad_c_one = jnp.sum(grad_first, axis=0)
    return (grad_v_one, grad_c_one, grad_v_two, grad_c_two, grad_v_three, grad_c_three)


def local(
    sensors,
    query_index,
    targets,
    w_one,
    b_one,
    w_two,
    b_two,
    v_one,
    c_one,
    v_two,
    c_two,
    v_three,
    c_three,
):
    dp_count, q_count = lax.axis_size("dp"), lax.axis_size("query")
    func_rows = sensors.shape[0]
    query_rows = query_index.shape[1]
    count_all = func_rows * dp_count * query_rows * q_count
    grad_scale = 64.0 / math.sqrt(count_all)
    inv_scale = 1.0 / math.sqrt(w_two.shape[1])
    dp_me, q_me = lax.axis_index("dp"), lax.axis_index("query")
    dp_bits, q_bits = bits_of(dp_count), bits_of(q_count)
    half = func_rows // 2
    parity = lax.rem(q_me, 2)
    mine = parity * half
    other = half - mine

    w_two_all, _ = gather_xor(w_two, "query", q_bits[::-1])
    sensor_cols = sensors.shape[1] // dp_count
    sensors_half = lax.dynamic_slice_in_dim(sensors, mine, half, 0)
    held = []
    for offset in range(dp_count):
        start = jnp.bitwise_xor(dp_me, offset) * sensor_cols
        block = lax.dynamic_slice_in_dim(sensors_half, start, sensor_cols, 1)
        held.append(block if offset == 0 else swap(block, "dp", offset))
    sensors_mine = jnp.concatenate(held, axis=0)
    sensors_other = swap(sensors_mine, "query", 1)

    hidden = jnp.tanh(jnp.dot(sensors, w_one, preferred_element_type=jnp.float32) + b_one)
    hidden_b = hidden.astype(jnp.bfloat16)
    hidden_all, _ = gather_xor(hidden_b, "query", q_bits[::-1])
    hidden_wide = jnp.concatenate(
        [hidden_all[i * func_rows : (i + 1) * func_rows] for i in range(q_count)], axis=1
    )

    coords = query_index.astype(jnp.float32) / (GRID - 1)
    first_act, first_b, second_act, second_b, basis_b = trunk_forward(
        coords, v_one, c_one, v_two, c_two, v_three, c_three
    )

    coeffs = jnp.dot(hidden_wide, w_two_all, preferred_element_type=jnp.float32) + b_two
    coeffs_b = coeffs.astype(jnp.bfloat16)
    prediction = contract_cols(coeffs_b, basis_b) * inv_scale
    misfit = prediction - targets.astype(jnp.float32)
    loss_part = jnp.sum(misfit * misfit)
    misfit_b = (misfit * grad_scale).astype(jnp.bfloat16)

    partial = jnp.dot(misfit_b, basis_b, preferred_element_type=jnp.float32) * inv_scale
    running = lax.dynamic_slice_in_dim(partial, mine, half, 0) + swap(
        lax.dynamic_slice_in_dim(partial, other, half, 0), "query", 1
    )
    for mask in q_bits[1:]:
        running = running + swap(running, "query", mask)
    running_b = running.astype(jnp.bfloat16)
    grad_coeffs_b = jnp.concatenate([running_b, swap(running_b, "query", 1)], axis=0)

    def in_order(value):
        return jnp.concatenate(
            [
                lax.dynamic_slice_in_dim(value, mine, half, 0),
                lax.dynamic_slice_in_dim(value, other, half, 0),
            ],
            axis=0,
        )

    hidden_o = in_order(hidden)
    hidden_bo = in_order(hidden_b)
    grad_pre = contract_cols(grad_coeffs_b, w_two) * (1.0 - hidden_o * hidden_o)
    grad_pre_b = grad_pre.astype(jnp.bfloat16)
    wide_first = dp_bits[1:][::-1] + dp_bits[:1]
    wide_last = dp_bits[:1] + dp_bits[1:][::-1]
    sides = []
    for rows, masks in ((grad_pre_b[:half], wide_first), (grad_pre_b[half:], wide_last)):
        blocks, offsets = gather_xor(rows, "dp", masks)
        sides.append(
            jnp.concatenate(
                [blocks[offsets.index(o) * half : (offsets.index(o) + 1) * half] for o in range(dp_count)],
                axis=0,
            )
        )
    grad_w_one = contract_rows(
        jnp.concatenate([sensors_mine, sensors_other], axis=0), jnp.concatenate(sides, axis=0)
    )

    rest = contract_rows(grad_coeffs_b, hidden_bo)
    bias_sum = jnp.broadcast_to(jnp.sum(grad_pre, axis=0)[None, :], (8, grad_pre.shape[1]))
    for mask in dp_bits[::-1]:
        rows = rest.shape[0] // 2
        upper = jnp.bitwise_and(dp_me, mask) // mask
        keep = lax.dynamic_slice_in_dim(rest, upper * rows, rows, 0)
        give = lax.dynamic_slice_in_dim(rest, (1 - upper) * rows, rows, 0)
        both = jnp.concatenate([keep, bias_sum], axis=0) + swap(
            jnp.concatenate([give, bias_sum], axis=0), "dp", mask
        )
        rest, bias_sum = both[:rows], both[rows:]
    grad_w_two = rest.T
    grad_b_one = bias_sum[0]

    trunk_parts = trunk_backward(
        coords, first_act, first_b, second_act, second_b, inv_scale * contract_rows(misfit_b, coeffs_b), v_two, v_three
    )
    width = w_two.shape[1]
    small = jnp.concatenate(
        [
            trunk_parts[0],
            trunk_parts[1][None],
            trunk_parts[3][None],
            trunk_parts[5][None],
            jnp.sum(partial, axis=0)[None],
            jnp.full((1, width), loss_part),
            jnp.zeros((1, width), jnp.float32),
        ],
        axis=0,
    )
    rows_two, rows_three = v_two.shape[0], v_three.shape[0]
    sums = lax.psum(
        jnp.concatenate([trunk_parts[2], trunk_parts[4], small], axis=0), ("dp", "query")
    )
    tail = sums[rows_two + rows_three :]
    return (
        tail[6, 0] / count_all,
        grad_w_one,
        grad_b_one,
        grad_w_two,
        tail[5],
        tail[0:2],
        tail[2],
        sums[:rows_two],
        tail[3],
        sums[rows_two : rows_two + rows_three],
        tail[4],
    )


def solution(mesh):
    placed = (
        P("dp", None),
        P(None, "query"),
        P("dp", "query"),
        P(None, "query"),
        P("query"),
        P("query", None),
        P(),
        P(),
        P(),
        P(),
        P(),
        P(),
        P(),
    )
    return jax.shard_map(
        local,
        mesh=mesh,
        in_specs=placed,
        out_specs=(
            P(),
            P("dp", "query"),
            P("query"),
            P("query", "dp"),
            P(),
            P(),
            P(),
            P(),
            P(),
            P(),
            P(),
        ),
        check_vma=False,
    )
```

```python
import math

import jax
import jax.numpy as jnp
from jax import lax
from jax.sharding import PartitionSpec as P

GRID = 128


def contract_rows(left, right, precision=None):
    return lax.dot_general(
        left,
        right,
        (((0,), (0,)), ((), ())),
        precision=precision,
        preferred_element_type=jnp.float32,
    )


def contract_cols(left, right, precision=None):
    return lax.dot_general(
        left,
        right,
        (((1,), (1,)), ((), ())),
        precision=precision,
        preferred_element_type=jnp.float32,
    )


def trunk_forward(coords, v_one, c_one, v_two, c_two, v_three, c_three):
    first_act = jnp.tanh(
        coords[0][:, None] * v_one[0][None, :] + coords[1][:, None] * v_one[1][None, :] + c_one
    )
    first_b = first_act.astype(jnp.bfloat16)
    second_act = jnp.tanh(jnp.dot(first_b, v_two, preferred_element_type=jnp.float32) + c_two)
    second_b = second_act.astype(jnp.bfloat16)
    basis_full = jnp.dot(second_b, v_three, preferred_element_type=jnp.float32) + c_three
    return (first_act, first_b, second_act, second_b, basis_full.astype(jnp.bfloat16))


def swap(value, axis, mask):
    count = lax.axis_size(axis)
    return lax.ppermute(value, axis, [(i, i ^ mask) for i in range(count)])


def bits_of(count):
    return [1 << b for b in range(count.bit_length() - 1)]


def gather_xor(value, axis, masks):
    blocks, offsets = value, [0]
    for mask in masks:
        blocks = jnp.concatenate([blocks, swap(blocks, axis, mask)], axis=0)
        offsets = offsets + [o ^ mask for o in offsets]
    return blocks, offsets


def split_pair(value):
    high = lax.reduce_precision(value, 8, 7)
    return high.astype(jnp.bfloat16), (value - high).astype(jnp.bfloat16)


def trunk_backward(coords, first_act, first_b, second_act, second_b, grad_basis, v_two, v_three):
    basis_hi, basis_lo = split_pair(grad_basis)
    grad_v_three = contract_rows(second_b, basis_hi) + contract_rows(second_b, basis_lo)
    grad_c_three = jnp.sum(grad_basis, axis=0)
    grad_second = (contract_cols(basis_hi, v_three) + contract_cols(basis_lo, v_three)) * (
        1.0 - second_act * second_act
    )
    second_hi, second_lo = split_pair(grad_second)
    grad_v_two = contract_rows(first_b, second_hi) + contract_rows(first_b, second_lo)
    grad_c_two = jnp.sum(grad_second, axis=0)
    grad_first = (contract_cols(second_hi, v_two) + contract_cols(second_lo, v_two)) * (
        1.0 - first_act * first_act
    )
    grad_v_one = jnp.stack(
        [jnp.sum(coords[0][:, None] * grad_first, axis=0), jnp.sum(coords[1][:, None] * grad_first, axis=0)]
    )
    grad_c_one = jnp.sum(grad_first, axis=0)
    return (grad_v_one, grad_c_one, grad_v_two, grad_c_two, grad_v_three, grad_c_three)


def local(
    sensors,
    query_index,
    targets,
    w_one,
    b_one,
    w_two,
    b_two,
    v_one,
    c_one,
    v_two,
    c_two,
    v_three,
    c_three,
):
    dp_count, q_count = lax.axis_size("dp"), lax.axis_size("query")
    func_rows = sensors.shape[0]
    query_rows = query_index.shape[1]
    count_all = func_rows * dp_count * query_rows * q_count
    grad_scale = 64.0 / math.sqrt(count_all)
    inv_scale = 1.0 / math.sqrt(w_two.shape[1])
    dp_me, q_me = lax.axis_index("dp"), lax.axis_index("query")
    dp_bits, q_bits = bits_of(dp_count), bits_of(q_count)
    half = func_rows // 2
    parity = lax.rem(q_me, 2)
    mine = parity * half
    other = half - mine

    w_two_all, _ = gather_xor(w_two, "query", q_bits[::-1])
    sensor_cols = sensors.shape[1] // dp_count
    sensors_half = lax.dynamic_slice_in_dim(sensors, mine, half, 0)
    held = []
    for offset in range(dp_count):
        start = jnp.bitwise_xor(dp_me, offset) * sensor_cols
        block = lax.dynamic_slice_in_dim(sensors_half, start, sensor_cols, 1)
        held.append(block if offset == 0 else swap(block, "dp", offset))
    sensors_mine = jnp.concatenate(held, axis=0)
    sensors_other = swap(sensors_mine, "query", 1)

    hidden = jnp.tanh(jnp.dot(sensors, w_one, preferred_element_type=jnp.float32) + b_one)
    hidden_b = hidden.astype(jnp.bfloat16)
    hidden_all, _ = gather_xor(hidden_b, "query", q_bits[::-1])
    hidden_wide = jnp.concatenate(
        [hidden_all[i * func_rows : (i + 1) * func_rows] for i in range(q_count)], axis=1
    )

    coords = query_index.astype(jnp.float32) / (GRID - 1)
    first_act, first_b, second_act, second_b, basis_b = trunk_forward(
        coords, v_one, c_one, v_two, c_two, v_three, c_three
    )

    coeffs = jnp.dot(hidden_wide, w_two_all, preferred_element_type=jnp.float32) + b_two
    coeffs_b = coeffs.astype(jnp.bfloat16)
    prediction = contract_cols(coeffs_b, basis_b) * inv_scale
    misfit = prediction - targets.astype(jnp.float32)
    loss_part = jnp.sum(misfit * misfit)
    misfit_b = (misfit * grad_scale).astype(jnp.bfloat16)

    partial = jnp.dot(misfit_b, basis_b, preferred_element_type=jnp.float32) * inv_scale
    running = lax.dynamic_slice_in_dim(partial, mine, half, 0) + swap(
        lax.dynamic_slice_in_dim(partial, other, half, 0), "query", 1
    )
    for mask in q_bits[1:]:
        running = running + swap(running, "query", mask)
    running_b = running.astype(jnp.bfloat16)
    grad_coeffs_b = jnp.concatenate([running_b, swap(running_b, "query", 1)], axis=0)

    def in_order(value):
        return jnp.concatenate(
            [
                lax.dynamic_slice_in_dim(value, mine, half, 0),
                lax.dynamic_slice_in_dim(value, other, half, 0),
            ],
            axis=0,
        )

    hidden_o = in_order(hidden)
    hidden_bo = in_order(hidden_b)
    grad_pre = contract_cols(grad_coeffs_b, w_two) * (1.0 - hidden_o * hidden_o)
    grad_pre_b = grad_pre.astype(jnp.bfloat16)
    wide_first = dp_bits[1:][::-1] + dp_bits[:1]
    wide_last = dp_bits[:1] + dp_bits[1:][::-1]
    sides = []
    for rows, masks in ((grad_pre_b[:half], wide_first), (grad_pre_b[half:], wide_last)):
        blocks, offsets = gather_xor(rows, "dp", masks)
        sides.append(
            jnp.concatenate(
                [blocks[offsets.index(o) * half : (offsets.index(o) + 1) * half] for o in range(dp_count)],
                axis=0,
            )
        )
    grad_w_one = contract_rows(
        jnp.concatenate([sensors_mine, sensors_other], axis=0), jnp.concatenate(sides, axis=0)
    )

    rest = contract_rows(grad_coeffs_b, hidden_bo)
    bias_sum = jnp.broadcast_to(jnp.sum(grad_pre, axis=0)[None, :], (8, grad_pre.shape[1]))
    for mask in dp_bits[::-1]:
        rows = rest.shape[0] // 2
        upper = jnp.bitwise_and(dp_me, mask) // mask
        keep = lax.dynamic_slice_in_dim(rest, upper * rows, rows, 0)
        give = lax.dynamic_slice_in_dim(rest, (1 - upper) * rows, rows, 0)
        both = jnp.concatenate([keep, bias_sum], axis=0) + swap(
            jnp.concatenate([give, bias_sum], axis=0), "dp", mask
        )
        rest, bias_sum = both[:rows], both[rows:]
    grad_w_two = rest.T
    grad_b_one = bias_sum[0]

    trunk_parts = trunk_backward(
        coords, first_act, first_b, second_act, second_b, inv_scale * contract_rows(misfit_b, coeffs_b), v_two, v_three
    )
    loss_sum, grad_b_two, *sums = lax.psum(
        (loss_part, jnp.sum(partial, axis=0)) + trunk_parts, ("dp", "query")
    )
    return (loss_sum / count_all, grad_w_one, grad_b_one, grad_w_two, grad_b_two, *sums)


def solution(mesh):
    placed = (
        P("dp", None),
        P(None, "query"),
        P("dp", "query"),
        P(None, "query"),
        P("query"),
        P("query", None),
        P(),
        P(),
        P(),
        P(),
        P(),
        P(),
        P(),
    )
    return jax.shard_map(
        local,
        mesh=mesh,
        in_specs=placed,
        out_specs=(
            P(),
            P("dp", "query"),
            P("query"),
            P("query", "dp"),
            P(),
            P(),
            P(),
            P(),
            P(),
            P(),
            P(),
        ),
        check_vma=False,
    )
```
